32 devices in a mesh: emit: 2 (over y), client: 16 (over z, x, core).
Axes of the slice: x: 2, y: 2, z: 4, core: 2. Of those that a mesh axis runs over, the one named last changes fastest.
Arguments:
- features: bfloat16 [65536, 768], P('client'), may hold values from -28 to 28
- labels: int32 [65536], P('client'), may hold values from 0 to 999
- client_ids: int32 [128], replicated, may hold values from 0 to 127, each once
- trunk_in: bfloat16 [128, 2048], replicated, may hold values from -6 to 6
- trunk_weight: bfloat16 [2048, 2048], P(None, 'client'), may hold values from -0.125 to 0.125
- class_table: bfloat16 [1000, 2048], P('emit'), may hold values from -6 to 6
- emit_weight: bfloat16 [2048, 768], P('emit'), may hold values from -0.125 to 0.125
Outputs:
- loss: float32 [65536], P('client')
- emit_grad: float32 [2048, 768], P(('emit', 'client'))
- trunk_grad: float32 [2048, 2048], P(None, ('emit', 'client'))
The draws below stay inside these ranges and needn't reach their ends.
Inputs may be any that keep to these rules, and one draw needn't show every extreme that they name: Each client number appears once; slot s holds the features of client client_ids[s].
All inputs are finite; a program needn't handle non-finite values.
Results may differ from the reference program's by a relative error of at most 0.022.
Values may be sent and summed in bfloat16 or wider, within the bound.
No kernel may reach another device: no remote copies, remote signals or barrier semaphores. Data moves between devices by JAX's collectives and lax.ppermute only.
A program may use at most 128 MiB of HBM per device.

```python
import jax
import jax.numpy as jnp
from jax import lax

FEAT = 768
HYPER = 2048
CLASSES = 1000
SAMPLES = 512
CLIENTS = 128


def draw_features(key, part):
    key_base = jax.random.fold_in(key, 11)
    base = jnp.clip(jax.random.normal(key_base, (CLIENTS * SAMPLES, FEAT), jnp.float32), -6.0, 6.0)
    return base.astype(jnp.bfloat16)


def set_ends(array, key, smallest, high):
    spot = [jax.random.randint(jax.random.fold_in(key, axis), (), 0, length) for axis, length in enumerate(array.shape)]
    main_axis = array.shape.index(max(array.shape))
    neighbour = spot[:main_axis] + [(spot[main_axis] + 1) % array.shape[main_axis]] + spot[main_axis + 1:]
    return array.at[tuple(spot)].set(smallest).at[tuple(neighbour)].set(high)


def block_scale(stream_key, dims, split, smallest, high):
    def one(axis_at, blocks):
        steps = jax.random.uniform(jax.random.fold_in(jax.random.fold_in(stream_key, 6), axis_at), (blocks,), jnp.float32, smallest / len(split), high / len(split))
        return jnp.repeat(jnp.exp(steps), dims[axis_at] // blocks).reshape((-1,) + (1,) * (len(dims) - axis_at - 1))

    level = one(*split[0])
    for cut in split[1:]:
        level = level * one(*cut)
    return level


def centred(stream_key, extent, deviation, reach, split=(), held_as=jnp.bfloat16):
    values = deviation * jax.random.normal(stream_key, extent, jnp.float32)
    if split:
        values = values * block_scale(stream_key, extent, split, -0.22, 0.18)
    return jnp.clip(values, -reach, reach).astype(held_as)


def setup_inputs(seed: int = 0) -> dict:
    seeds = jax.random.split(jax.random.key(seed), 8)
    features = draw_features(jax.random.fold_in(seeds[7], 71), 0)
    labels = set_ends(jax.random.randint(seeds[1], (CLIENTS * SAMPLES,), 0, CLASSES), jax.random.fold_in(seeds[1], 1), 0, CLASSES - 1).astype(jnp.int32)
    client_ids = jax.random.permutation(seeds[2], CLIENTS).astype(jnp.int32)
    trunk_in = centred(seeds[3], (CLIENTS, HYPER), 1.0, 6.0)
    trunk_weight = centred(seeds[4], (HYPER, HYPER), HYPER ** -0.5, 0.125, ((1, 16),))
    class_table = centred(seeds[5], (CLASSES, HYPER), 1.0, 6.0, ((0, 2),))
    emit_weight = centred(seeds[6], (HYPER, FEAT), HYPER ** -0.5, 0.125, ((0, 2),))
    return {"features": features, "labels": labels, "client_ids": client_ids, "trunk_in": trunk_in, "trunk_weight": trunk_weight, "class_table": class_table, "emit_weight": emit_weight}


def silu_grad(value):
    sig = jax.nn.sigmoid(value)
    return sig * (1.0 + value * (1.0 - sig))

def reference(features, labels, client_ids, trunk_in, trunk_weight, class_table, emit_weight):
    pre = jnp.dot(trunk_in, trunk_weight, preferred_element_type=jnp.float32).astype(jnp.bfloat16)
    pre_slots = pre[client_ids.astype(jnp.int32)].astype(jnp.float32)
    feats = features.reshape(CLIENTS, SAMPLES, FEAT)
    labs = labels.reshape(CLIENTS, SAMPLES)
    table = class_table.astype(jnp.float32)
    classes = jnp.arange(CLASSES, dtype=jnp.int32)

    def per_slot(carry, item):
        pre_row, feat, lab = item
        code_in = jax.nn.silu(pre_row)[None, :] + table
        code = jax.nn.silu(code_in).astype(jnp.bfloat16)
        heads = jnp.dot(code, emit_weight, preferred_element_type=jnp.float32).astype(jnp.bfloat16)
        logits = jnp.dot(feat, heads.T, preferred_element_type=jnp.float32)
        top = lax.optimization_barrier(jnp.max(logits, axis=1, keepdims=True))
        expd = jnp.exp(logits - top)
        total = lax.optimization_barrier(jnp.sum(expd, axis=1, keepdims=True))
        onehot = (lab[:, None] == classes[None, :]).astype(jnp.float32)
        loss = top[:, 0] + jnp.log(total[:, 0]) - lax.optimization_barrier(jnp.sum(logits * onehot, axis=1))
        grad_logits = ((expd / total - onehot) / CLIENTS).astype(jnp.bfloat16)
        grad_heads = jnp.dot(grad_logits.T, feat, preferred_element_type=jnp.float32).astype(jnp.bfloat16)
        carry = carry + jnp.dot(code.T, grad_heads, preferred_element_type=jnp.float32)
        grad_code = jnp.dot(grad_heads, emit_weight.T, preferred_element_type=jnp.float32)
        grad_sum = lax.optimization_barrier(jnp.sum(grad_code * silu_grad(code_in), axis=0))
        grad_pre = (grad_sum * silu_grad(pre_row)).astype(jnp.bfloat16)
        return (carry, (loss, grad_pre))
    emit_grad, (loss, grad_pre) = lax.scan(per_slot, jnp.zeros((HYPER, FEAT), jnp.float32), (pre_slots, feats, labs))
    grad_client = jnp.zeros((CLIENTS, HYPER), jnp.bfloat16).at[client_ids.astype(jnp.int32)].set(grad_pre)
    trunk_grad = jnp.dot(trunk_in.T, grad_client, preferred_element_type=jnp.float32)
    return (loss.reshape(CLIENTS * SAMPLES), emit_grad, trunk_grad)
```

```python
import functools

import jax
import jax.numpy as jnp
from jax import lax
from jax.experimental import pallas as pl
from jax.experimental.pallas import tpu as pltpu
from jax.sharding import PartitionSpec as P

MIB = 1024 * 1024


def params(mib):
    return pltpu.CompilerParams(vmem_limit_bytes=mib * MIB)


def matmul_cost(m, k, n, nbytes):
    return pl.CostEstimate(flops=2 * m * k * n, bytes_accessed=nbytes, transcendentals=0)


def silu_grad(value):
    sig = jax.nn.sigmoid(value)
    return sig * (1.0 + value * (1.0 - sig))


def code_kernel(classes, act_ref, table_ref, code_ref, slope_ref, half_ref):
    @pl.when(pl.program_id(0) == 0)
    def _():
        number = lax.broadcasted_iota(jnp.int32, half_ref.shape, 0)
        half = 0.5 * table_ref[...].astype(jnp.float32)
        half_ref[...] = jnp.where(number < classes, half, 0.0)

    y = act_ref[0] + half_ref[...]
    th = jnp.tanh(y)
    up = 1.0 + th
    code_ref[...] = (y * up).astype(jnp.bfloat16)
    slope_ref[...] = (up * (1.0 + y * (1.0 - th))).astype(jnp.bfloat16)


def forward_kernel(classes, where_ref, code_ref, local_ref, mine_ref, theirs_ref, feat_ref, label_ref, p_ref, stat_ref, emit_ref, heads_ref):
    rows, samples = p_ref.shape

    @pl.when(pl.program_id(0) == 0)
    def _():
        size = local_ref.shape[0]
        half = size // 2
        emit_index, core = where_ref[0], where_ref[1]
        emit_ref[pl.ds(pl.multiple_of(emit_index * size, size), size), :] = local_ref[...]
        for j in range(mine_ref.shape[0]):
            base = (emit_index ^ (j + 1)) * size
            first = pl.multiple_of(base + core * half, half)
            second = pl.multiple_of(base + (1 - core) * half, half)
            emit_ref[pl.ds(first, half), :] = mine_ref[j]
            emit_ref[pl.ds(second, half), :] = theirs_ref[j]

    step, last = pl.program_id(0), pl.num_programs(0) - 1

    def make_heads():
        return jnp.dot(
            code_ref[...], emit_ref[...], preferred_element_type=jnp.float32
        ).astype(jnp.bfloat16)

    def make_logits():
        return lax.dot_general(
            heads_ref[...], feat_ref[...], (((1,), (1,)), ((), ())),
            preferred_element_type=jnp.float32,
        )

    def soften(logits):
        number = lax.broadcasted_iota(jnp.int32, (rows, samples), 0)
        target = jnp.sum(jnp.where(number == label_ref[0], logits, 0.0), axis=0, keepdims=True)
        logits = jnp.where(number < classes, logits, -jnp.inf)
        top = jnp.max(logits, axis=0, keepdims=True)
        p = jnp.exp(logits - top)
        p_ref[...] = p
        stat_ref[0, 0:1, :] = top
        stat_ref[0, 1:2, :] = jnp.sum(p, axis=0, keepdims=True)
        stat_ref[0, 2:3, :] = target

    @pl.when(step == 0)
    def _():
        heads_ref[...] = make_heads()

    @pl.when((step > 0) & (step < last))
    def _():
        logits = make_logits()
        heads = make_heads()
        soften(logits)
        heads_ref[...] = heads

    @pl.when(step == last)
    def _():
        soften(make_logits())


def store_emit_grad(block, is_first, code, gh, keep_ref, send_ref):
    acc = lax.dot_general(code, gh, (((0,), (0,)), ((), ())), preferred_element_type=jnp.float32)
    width, feat_dim = acc.shape
    acc = acc.reshape(width // (2 * block), 2, block, feat_dim)
    first, second = acc[:, 0].reshape(width // 2, feat_dim), acc[:, 1].reshape(width // 2, feat_dim)
    keep_ref[...] = jnp.where(is_first, first, second).astype(jnp.bfloat16)
    send_ref[...] = jnp.where(is_first, second, first).astype(jnp.bfloat16)


def head_grad_kernel(inv_clients, block, slots, where_ref, p_ref, scale_ref, label_ref, feat_ref, code_ref, gh_ref, keep_ref, send_ref, all_ref):
    step = pl.program_id(0)
    rows = p_ref.shape[0]

    @pl.when(step < slots)
    def _():
        number = lax.broadcasted_iota(jnp.int32, p_ref.shape, 0)
        soft = p_ref[...] * scale_ref[0]
        grad = (soft - jnp.where(number == label_ref[0], 1.0, 0.0)) * inv_clients
        gh = jnp.dot(
            grad.astype(jnp.bfloat16), feat_ref[...], preferred_element_type=jnp.float32
        ).astype(jnp.bfloat16)
        gh_ref[...] = gh
        all_ref[pl.ds(pl.multiple_of(step * rows, rows), rows), :] = gh

    @pl.when(step >= slots)
    def _():
        store_emit_grad(block, where_ref[1] == 0, code_ref[...], all_ref[...], keep_ref, send_ref)


def store_code_grad(gh, slope_ref, emit_ref, pre_slope_ref, out_ref):
    hidden = emit_ref.shape[0]
    width = min(512, hidden)
    for c in range(hidden // width):
        cols = slice(c * width, (c + 1) * width)
        grad_code = lax.dot_general(
            gh, emit_ref[cols, :], (((1,), (1,)), ((), ())), preferred_element_type=jnp.float32
        )
        slope = slope_ref[:, cols].astype(jnp.float32)
        grad_sum = 0.5 * jnp.sum(grad_code * slope, axis=0, keepdims=True)
        out_ref[0, :, cols] = (grad_sum * pre_slope_ref[0, :, cols]).astype(out_ref.dtype)


def code_grad_kernel(slope_ref, emit_ref, pre_slope_ref, gh_ref, out_ref):
    store_code_grad(gh_ref[...], slope_ref, emit_ref, pre_slope_ref, out_ref)


def both_grads_kernel(block, count, slots, where_ref, slope_ref, emit_ref, pre_slope_ref, gh_ref, code_ref, out_ref, keep_ref, send_ref, all_ref):
    step = pl.program_id(0)
    rows = slope_ref.shape[0]

    @pl.when(step < count)
    def _():
        store_code_grad(gh_ref[...], slope_ref, emit_ref, pre_slope_ref, out_ref)

    @pl.when(step < slots)
    def _():
        all_ref[pl.ds(pl.multiple_of(step * rows, rows), rows), :] = gh_ref[...]

    @pl.when(step >= slots)
    def _():
        store_emit_grad(block, where_ref[1] == 0, code_ref[...], all_ref[...], keep_ref, send_ref)


def xor_pairs(size, bit):
    return [(i, i ^ bit) for i in range(size)]


def bits_of(size):
    return [1 << b for b in range(size.bit_length() - 1)]


def gather_emit(local, client_index):
    emits, clients = lax.axis_size("emit"), lax.axis_size("client")
    core = client_index & 1
    half = local.shape[0] // 2
    mine = lax.dynamic_slice_in_dim(local, core * half, half)[None]
    for bit in bits_of(emits):
        mine = jnp.concatenate([mine, lax.ppermute(mine, "emit", xor_pairs(emits, bit))])
    theirs = lax.ppermute(mine[1:], "client", xor_pairs(clients, 1))
    return mine[1:], theirs


def halve(value, dim, axis, size, bit, index):
    own = jnp.where((index & bit) != 0, 1, 0)
    send = lax.dynamic_index_in_dim(value, 1 - own, dim, keepdims=False)
    keep = lax.dynamic_index_in_dim(value, own, dim, keepdims=False)
    got = lax.ppermute(send, axis, xor_pairs(size, bit))
    return (keep.astype(jnp.float32) + got.astype(jnp.float32)).astype(jnp.bfloat16)


def per_device(features, labels, client_ids, trunk_in, trunk_weight, class_table, emit_weight):
    emits, client_size = lax.axis_size("emit"), lax.axis_size("client")
    clients, hidden = trunk_in.shape
    slots = clients // client_size
    classes = class_table.shape[0]
    feat_dim = features.shape[1]
    samples = features.shape[0] // slots
    rows = -(-classes // 128) * 128
    client_index = lax.axis_index("client")
    emit_index = lax.axis_index("emit")
    f32, bf16 = jnp.float32, jnp.bfloat16

    where = jnp.stack([emit_index, client_index & 1, emit_index // (emits // 2)]).astype(jnp.int32)
    pre_cols = jnp.dot(trunk_in, trunk_weight, preferred_element_type=f32).astype(bf16)
    numbers = lax.iota(jnp.int32, clients)
    picker = (client_ids[:, None] == numbers[None, :]).astype(bf16)
    pre_slots = jnp.dot(picker, pre_cols, preferred_element_type=f32).astype(bf16)
    pre_slots, emit_source = lax.optimization_barrier((pre_slots, emit_weight))
    pre_own = lax.all_to_all(
        pre_slots.reshape(client_size, slots, hidden // client_size), "client", 0, 0
    )
    pre_own = pre_own.transpose(1, 0, 2).reshape(slots, hidden).astype(f32)
    mine, theirs = gather_emit(emit_source, client_index)
    act = (0.5 * jax.nn.silu(pre_own))[:, None, :]
    pre_slope = silu_grad(pre_own)[:, None, :]
    local = labels - emit_index * classes
    local = jnp.where((local >= 0) & (local < classes), local, -1).reshape(slots, 1, samples)

    half = emit_weight.shape[0] // 2
    before = lambda s: jnp.maximum(s - 1, 0)
    once = dict(pipeline_mode=pl.Buffered(1))
    whole = lambda shape: pl.BlockSpec(shape, lambda s, *_: (0,) * len(shape), **once)
    per_slot = lambda shape: pl.BlockSpec((1,) + shape, lambda s, *_: (s, 0, 0))
    row_block = lambda shape: pl.BlockSpec(shape, lambda s, *_: (s, 0))
    make_code = pl.pallas_call(
        functools.partial(code_kernel, classes),
        grid=(slots,),
        in_specs=[per_slot((1, hidden)), whole((rows, hidden))],
        out_specs=[row_block((rows, hidden)), row_block((rows, hidden))],
        out_shape=[pltpu.HBM((slots * rows, hidden), bf16)] * 2,
        scratch_shapes=[pltpu.VMEM((rows, hidden), f32)],
        compiler_params=params(58),
        cost_estimate=pl.CostEstimate(
            flops=int(4e9), bytes_accessed=4 * slots * rows * hidden, transcendentals=0
        ),
        name="code",
    )
    code, slope = make_code(act, class_table)

    p, stats, emit_full = pl.pallas_call(
        functools.partial(forward_kernel, classes),
        grid_spec=pltpu.PrefetchScalarGridSpec(
            num_scalar_prefetch=1,
            grid=(slots + 1,),
            in_specs=[
                pl.BlockSpec((rows, hidden), lambda s, *_: (jnp.minimum(s, slots - 1), 0)),
                whole(emit_weight.shape),
                whole((emits - 1, half, feat_dim)),
                whole((emits - 1, half, feat_dim)),
                pl.BlockSpec((samples, feat_dim), lambda s, *_: (before(s), 0)),
                pl.BlockSpec((1, 1, samples), lambda s, *_: (before(s), 0, 0)),
            ],
            out_specs=[
                pl.BlockSpec((rows, samples), lambda s, *_: (before(s), 0)),
                pl.BlockSpec((1, 3, samples), lambda s, *_: (before(s), 0, 0)),
                pl.BlockSpec((hidden, feat_dim), lambda s, *_: (0, 0)),
            ],
            scratch_shapes=[pltpu.VMEM((rows, feat_dim), bf16)],
        ),
        out_shape=[
            jax.ShapeDtypeStruct((slots * rows, samples), f32),
            pltpu.HBM((slots, 3, samples), f32),
            pltpu.HBM((hidden, feat_dim), bf16),
        ],
        compiler_params=params(58),
        cost_estimate=matmul_cost(slots * rows, hidden + samples, feat_dim, 30 * MIB),
        name="forward",
    )(where, code, emit_weight, mine, theirs, features, local)

    top, total, target = stats[:, 0], stats[:, 1], stats[:, 2]
    for bit in bits_of(emits):
        other = lax.ppermute(jnp.stack([top, total, target], 1), "emit", xor_pairs(emits, bit))
        new_top = jnp.maximum(top, other[:, 0])
        total = total * jnp.exp(top - new_top) + other[:, 1] * jnp.exp(other[:, 0] - new_top)
        target = target + other[:, 2]
        top = new_top
    loss = (top + jnp.log(total) - target).reshape(slots * samples)
    scale = (jnp.exp(stats[:, 0] - top) / total)[:, None, :]

    block = hidden // (emits * client_size)
    width = min(256, hidden // 2)
    steps = hidden // 2 // width
    halves = [jax.ShapeDtypeStruct((hidden // 4, feat_dim), bf16)] * 2
    at = lambda bit: jnp.stack([bit * steps, where[1]]).astype(jnp.int32)
    slot_of = lambda s: jnp.minimum(s, slots - 1)
    step_of = lambda s: jnp.maximum(s - slots, 0)

    gh, keep_a, send_a = pl.pallas_call(
        functools.partial(head_grad_kernel, 1.0 / clients, block, slots),
        grid_spec=pltpu.PrefetchScalarGridSpec(
            num_scalar_prefetch=1,
            grid=(slots + steps,),
            in_specs=[
                pl.BlockSpec((rows, samples), lambda s, w: (slot_of(s), 0)),
                pl.BlockSpec((1, 1, samples), lambda s, w: (slot_of(s), 0, 0)),
                pl.BlockSpec((1, 1, samples), lambda s, w: (slot_of(s), 0, 0)),
                pl.BlockSpec((samples, feat_dim), lambda s, w: (slot_of(s), 0)),
                pl.BlockSpec((slots * rows, width), lambda s, w: (0, w[0] + step_of(s))),
            ],
            out_specs=[pl.BlockSpec((rows, feat_dim), lambda s, w: (slot_of(s), 0))]
            + [pl.BlockSpec((width // 2, feat_dim), lambda s, w: (step_of(s), 0))] * 2,
            scratch_shapes=[pltpu.VMEM((slots * rows, feat_dim), bf16)],
        ),
        out_shape=[pltpu.HBM((slots * rows, feat_dim), bf16)] + halves,
        compiler_params=params(58),
        cost_estimate=matmul_cost(feat_dim, slots * rows, hidden // 2 + samples, 20 * MIB),
        name="head_grad",
    )(at(1 - where[2]), p, scale, local, features, code)

    def both_grads(count, gh, code):
        early_of = lambda s: jnp.minimum(s, count - 1)
        return pl.pallas_call(
            functools.partial(both_grads_kernel, block, count, slots),
            grid_spec=pltpu.PrefetchScalarGridSpec(
                num_scalar_prefetch=1,
                grid=(slots + steps,),
                in_specs=[
                    pl.BlockSpec((rows, hidden), lambda s, w: (early_of(s), 0)),
                    whole((hidden, feat_dim)),
                    pl.BlockSpec((1, 1, hidden), lambda s, w: (early_of(s), 0, 0)),
                    pl.BlockSpec((rows, feat_dim), lambda s, w: (slot_of(s), 0)),
                    pl.BlockSpec((slots * rows, width), lambda s, w: (0, w[0] + step_of(s))),
                ],
                out_specs=[pl.BlockSpec((1, 1, hidden), lambda s, w: (early_of(s), 0, 0))]
                + [pl.BlockSpec((width // 2, feat_dim), lambda s, w: (step_of(s), 0))] * 2,
                scratch_shapes=[pltpu.VMEM((slots * rows, feat_dim), bf16)],
            ),
            out_shape=[jax.ShapeDtypeStruct((count, 1, hidden), bf16)] + halves,
            compiler_params=params(58),
            cost_estimate=matmul_cost(
                feat_dim, slots * rows, hidden // 2 + hidden * count // slots, 30 * MIB
            ),
            name="both_grads",
        )(at(where[2]), slope, emit_full, pre_slope, gh, code)

    def code_grad(first, count, gh):
        return pl.pallas_call(
            code_grad_kernel,
            grid=(count,),
            in_specs=[
                pl.BlockSpec((rows, hidden), lambda s: (s + first, 0)),
                whole((hidden, feat_dim)),
                pl.BlockSpec((1, 1, hidden), lambda s: (s + first, 0, 0)),
                pl.BlockSpec((rows, feat_dim), lambda s: (s + first, 0)),
            ],
            out_specs=per_slot((1, hidden)),
            out_shape=jax.ShapeDtypeStruct((count, 1, hidden), bf16),
            compiler_params=params(58),
            cost_estimate=matmul_cost(count * rows, feat_dim, hidden, 3 * count * MIB),
            name="code_grad",
        )(slope, emit_full, pre_slope, gh)

    add = lambda *terms: sum(t.astype(f32) for t in terms).astype(bf16)
    swap_core = lambda v: lax.ppermute(v, "client", xor_pairs(client_size, 1))
    top_bit = emits // 2
    got_a = swap_core(send_a)
    sum_a = add(keep_a, got_a)
    sum_a, code, gh = lax.optimization_barrier((sum_a, code, gh))
    from_pair = lax.ppermute(sum_a, "emit", xor_pairs(emits, top_bit))
    early = (slots * 3) // 4
    early_sum, keep_b, send_b = both_grads(early, gh, code)
    value = add(keep_b, swap_core(send_b), from_pair)
    value, gh = lax.optimization_barrier((value, gh))
    grad_pre = jnp.concatenate([early_sum, code_grad(early, slots - early, gh)])[:, 0]

    emit_bits, client_bits = bits_of(emits)[:-1][::-1], bits_of(client_size)[1:]
    value = value.reshape((2,) * (len(emit_bits) + len(client_bits)) + (block, feat_dim))
    for bit in emit_bits:
        value = halve(value, 0, "emit", emits, bit, emit_index)
    value = halve(value, value.ndim - 3, "client", client_size, client_bits[0], client_index)
    blocks = grad_pre.reshape(slots, emits * client_size, block).transpose(1, 0, 2)
    blocks, value = lax.optimization_barrier((blocks, value))
    value = value.reshape(client_size // 4, block, feat_dim)
    own = client_index // 4
    pieces = [lax.dynamic_index_in_dim(value, own, 0, keepdims=False)]
    for k in range(1, client_size // 4):
        send = lax.dynamic_index_in_dim(value, own ^ k, 0, keepdims=False)
        pieces.append(lax.ppermute(send, "client", xor_pairs(client_size, 4 * k)))
    value = sum(piece.astype(f32) for piece in pieces)
    emit_grad = value

    got = lax.all_to_all(blocks, ("emit", "client"), 0, 0)
    got = got.reshape(emits, clients, block).astype(f32)
    grad_slots = jnp.sum(got, axis=0).astype(bf16)
    grad_client = lax.dot_general(
        picker, grad_slots, (((0,), (0,)), ((), ())), preferred_element_type=f32
    ).astype(bf16)
    trunk_grad = lax.dot_general(
        trunk_in, grad_client, (((0,), (0,)), ((), ())), preferred_element_type=f32
    )
    return (loss, emit_grad, trunk_grad)


def solution(mesh):
    return jax.shard_map(
        per_device,
        mesh=mesh,
        in_specs=(
            P("client", None),
            P("client"),
            P(),
            P(),
            P(None, "client"),
            P("emit", None),
            P("emit", None),
        ),
        out_specs=(P("client"), P(("emit", "client"), None), P(None, ("emit", "client"))),
        check_vma=False,
    )
```

```python
import functools

import jax
import jax.numpy as jnp
from jax import lax
from jax.experimental import pallas as pl
from jax.experimental.pallas import tpu as pltpu
from jax.sharding import PartitionSpec as P

MIB = 1024 * 1024


def params(mib):
    return pltpu.CompilerParams(vmem_limit_bytes=mib * MIB)


def matmul_cost(m, k, n, nbytes):
    return pl.CostEstimate(flops=2 * m * k * n, bytes_accessed=nbytes, transcendentals=0)


def silu_grad(value):
    sig = jax.nn.sigmoid(value)
    return sig * (1.0 + value * (1.0 - sig))


def code_kernel(classes, act_ref, table_ref, code_ref, slope_ref, half_ref):
    @pl.when(pl.program_id(0) == 0)
    def _():
        number = lax.broadcasted_iota(jnp.int32, half_ref.shape, 0)
        half = 0.5 * table_ref[...].astype(jnp.float32)
        half_ref[...] = jnp.where(number < classes, half, 0.0)

    y = act_ref[0] + half_ref[...]
    th = jnp.tanh(y)
    up = 1.0 + th
    code_ref[...] = (y * up).astype(jnp.bfloat16)
    slope_ref[...] = (up * (1.0 + y * (1.0 - th))).astype(jnp.bfloat16)


def forward_kernel(classes, where_ref, code_ref, local_ref, mine_ref, theirs_ref, feat_ref, label_ref, p_ref, stat_ref, emit_ref, heads_ref):
    rows, samples = p_ref.shape

    @pl.when(pl.program_id(0) == 0)
    def _():
        size = local_ref.shape[0]
        half = size // 2
        emit_index, core = where_ref[0], where_ref[1]
        emit_ref[pl.ds(pl.multiple_of(emit_index * size, size), size), :] = local_ref[...]
        for j in range(mine_ref.shape[0]):
            base = (emit_index ^ (j + 1)) * size
            first = pl.multiple_of(base + core * half, half)
            second = pl.multiple_of(base + (1 - core) * half, half)
            emit_ref[pl.ds(first, half), :] = mine_ref[j]
            emit_ref[pl.ds(second, half), :] = theirs_ref[j]

    step, last = pl.program_id(0), pl.num_programs(0) - 1

    def make_heads():
        return jnp.dot(
            code_ref[...], emit_ref[...], preferred_element_type=jnp.float32
        ).astype(jnp.bfloat16)

    def make_logits():
        return lax.dot_general(
            heads_ref[...], feat_ref[...], (((1,), (1,)), ((), ())),
            preferred_element_type=jnp.float32,
        )

    def soften(logits):
        number = lax.broadcasted_iota(jnp.int32, (rows, samples), 0)
        target = jnp.sum(jnp.where(number == label_ref[0], logits, 0.0), axis=0, keepdims=True)
        logits = jnp.where(number < classes, logits, -jnp.inf)
        top = jnp.max(logits, axis=0, keepdims=True)
        p = jnp.exp(logits - top)
        p_ref[...] = p.astype(jnp.bfloat16)
        stat_ref[0, 0:1, :] = top
        stat_ref[0, 1:2, :] = jnp.sum(p, axis=0, keepdims=True)
        stat_ref[0, 2:3, :] = target

    @pl.when(step == 0)
    def _():
        heads_ref[...] = make_heads()

    @pl.when((step > 0) & (step < last))
    def _():
        logits = make_logits()
        heads = make_heads()
        soften(logits)
        heads_ref[...] = heads

    @pl.when(step == last)
    def _():
        soften(make_logits())


def store_emit_grad(block, is_first, code, gh, keep_ref, send_ref):
    acc = lax.dot_general(code, gh, (((0,), (0,)), ((), ())), preferred_element_type=jnp.float32)
    width, feat_dim = acc.shape
    acc = acc.reshape(width // (2 * block), 2, block, feat_dim)
    first, second = acc[:, 0].reshape(width // 2, feat_dim), acc[:, 1].reshape(width // 2, feat_dim)
    keep_ref[...] = jnp.where(is_first, first, second).astype(jnp.bfloat16)
    send_ref[...] = jnp.where(is_first, second, first).astype(jnp.bfloat16)


def head_grad_kernel(block, slots, where_ref, p_ref, scale_ref, at_label_ref, label_ref, feat_ref, code_ref, gh_ref, keep_ref, send_ref, all_ref):
    step = pl.program_id(0)
    rows = p_ref.shape[0]

    @pl.when(step < slots)
    def _():
        number = lax.broadcasted_iota(jnp.int32, p_ref.shape, 0)
        grad = p_ref[...].astype(jnp.float32) * scale_ref[0]
        grad = jnp.where(number == label_ref[0], at_label_ref[0], grad)
        gh = jnp.dot(
            grad.astype(jnp.bfloat16), feat_ref[...], preferred_element_type=jnp.float32
        ).astype(jnp.bfloat16)
        gh_ref[...] = gh
        all_ref[pl.ds(pl.multiple_of(step * rows, rows), rows), :] = gh

    @pl.when(step >= slots)
    def _():
        store_emit_grad(block, where_ref[1] == 0, code_ref[...], all_ref[...], keep_ref, send_ref)


def store_code_grad(gh, slope_ref, emit_ref, pre_slope_ref, out_ref):
    hidden = emit_ref.shape[0]
    width = min(512, hidden)
    for c in range(hidden // width):
        cols = slice(c * width, (c + 1) * width)
        grad_code = lax.dot_general(
            gh, emit_ref[cols, :], (((1,), (1,)), ((), ())), preferred_element_type=jnp.float32
        )
        slope = slope_ref[:, cols].astype(jnp.float32)
        grad_sum = 0.5 * jnp.sum(grad_code * slope, axis=0, keepdims=True)
        out_ref[0, :, cols] = (grad_sum * pre_slope_ref[0, :, cols]).astype(out_ref.dtype)


def code_grad_kernel(slope_ref, emit_ref, pre_slope_ref, gh_ref, out_ref):
    store_code_grad(gh_ref[...], slope_ref, emit_ref, pre_slope_ref, out_ref)


def emit_grad_kernel(block, where_ref, gh_ref, code_ref, keep_ref, send_ref):
    store_emit_grad(block, where_ref[1] == 0, code_ref[...], gh_ref[...], keep_ref, send_ref)


def xor_pairs(size, bit):
    return [(i, i ^ bit) for i in range(size)]


def bits_of(size):
    return [1 << b for b in range(size.bit_length() - 1)]


def gather_emit(local, client_index):
    emits, clients = lax.axis_size("emit"), lax.axis_size("client")
    core = client_index & 1
    half = local.shape[0] // 2
    mine = lax.dynamic_slice_in_dim(local, core * half, half)[None]
    for bit in bits_of(emits):
        mine = jnp.concatenate([mine, lax.ppermute(mine, "emit", xor_pairs(emits, bit))])
    theirs = lax.ppermute(mine[1:], "client", xor_pairs(clients, 1))
    return mine[1:], theirs


def halve(value, dim, axis, size, bit, index):
    own = jnp.where((index & bit) != 0, 1, 0)
    send = lax.dynamic_index_in_dim(value, 1 - own, dim, keepdims=False)
    keep = lax.dynamic_index_in_dim(value, own, dim, keepdims=False)
    got = lax.ppermute(send, axis, xor_pairs(size, bit))
    return (keep.astype(jnp.float32) + got.astype(jnp.float32)).astype(jnp.bfloat16)


def per_device(features, labels, client_ids, trunk_in, trunk_weight, class_table, emit_weight):
    emits, client_size = lax.axis_size("emit"), lax.axis_size("client")
    clients, hidden = trunk_in.shape
    slots = clients // client_size
    classes = class_table.shape[0]
    feat_dim = features.shape[1]
    samples = features.shape[0] // slots
    rows = -(-classes // 128) * 128
    client_index = lax.axis_index("client")
    emit_index = lax.axis_index("emit")
    f32, bf16 = jnp.float32, jnp.bfloat16

    where = jnp.stack([emit_index, client_index & 1, emit_index // (emits // 2)]).astype(jnp.int32)
    pre_cols = jnp.dot(trunk_in, trunk_weight, preferred_element_type=f32).astype(bf16)
    numbers = lax.iota(jnp.int32, clients)
    picker = (client_ids[:, None] == numbers[None, :]).astype(bf16)
    pre_slots = jnp.dot(picker, pre_cols, preferred_element_type=f32).astype(bf16)
    pre_slots, emit_source = lax.optimization_barrier((pre_slots, emit_weight))
    pre_own = lax.all_to_all(
        pre_slots.reshape(client_size, slots, hidden // client_size), "client", 0, 0
    )
    pre_own = pre_own.transpose(1, 0, 2).reshape(slots, hidden).astype(f32)
    mine, theirs = gather_emit(emit_source, client_index)
    act = (0.5 * jax.nn.silu(pre_own))[:, None, :]
    pre_slope = silu_grad(pre_own)[:, None, :]
    local = labels - emit_index * classes
    local = jnp.where((local >= 0) & (local < classes), local, -1).reshape(slots, 1, samples)

    half = emit_weight.shape[0] // 2
    before = lambda s: jnp.maximum(s - 1, 0)
    once = dict(pipeline_mode=pl.Buffered(1))
    whole = lambda shape: pl.BlockSpec(shape, lambda s, *_: (0,) * len(shape), **once)
    per_slot = lambda shape: pl.BlockSpec((1,) + shape, lambda s, *_: (s, 0, 0))
    row_block = lambda shape: pl.BlockSpec(shape, lambda s, *_: (s, 0))
    make_code = pl.pallas_call(
        functools.partial(code_kernel, classes),
        grid=(slots,),
        in_specs=[per_slot((1, hidden)), whole((rows, hidden))],
        out_specs=[row_block((rows, hidden)), row_block((rows, hidden))],
        out_shape=[pltpu.HBM((slots * rows, hidden), bf16)] * 2,
        scratch_shapes=[pltpu.VMEM((rows, hidden), f32)],
        compiler_params=params(58),
        cost_estimate=pl.CostEstimate(
            flops=int(4e9), bytes_accessed=4 * slots * rows * hidden, transcendentals=0
        ),
        name="code",
    )
    code, slope = make_code(act, class_table)

    p, stats, emit_full = pl.pallas_call(
        functools.partial(forward_kernel, classes),
        grid_spec=pltpu.PrefetchScalarGridSpec(
            num_scalar_prefetch=1,
            grid=(slots + 1,),
            in_specs=[
                pl.BlockSpec((rows, hidden), lambda s, *_: (jnp.minimum(s, slots - 1), 0)),
                whole(emit_weight.shape),
                whole((emits - 1, half, feat_dim)),
                whole((emits - 1, half, feat_dim)),
                pl.BlockSpec((samples, feat_dim), lambda s, *_: (before(s), 0)),
                pl.BlockSpec((1, 1, samples), lambda s, *_: (before(s), 0, 0)),
            ],
            out_specs=[
                pl.BlockSpec((rows, samples), lambda s, *_: (before(s), 0)),
                pl.BlockSpec((1, 3, samples), lambda s, *_: (before(s), 0, 0)),
                pl.BlockSpec((hidden, feat_dim), lambda s, *_: (0, 0)),
            ],
            scratch_shapes=[pltpu.VMEM((rows, feat_dim), bf16)],
        ),
        out_shape=[
            jax.ShapeDtypeStruct((slots * rows, samples), bf16),
            pltpu.HBM((slots, 3, samples), f32),
            pltpu.HBM((hidden, feat_dim), bf16),
        ],
        compiler_params=params(58),
        cost_estimate=matmul_cost(slots * rows, hidden + samples, feat_dim, 30 * MIB),
        name="forward",
    )(where, code, emit_weight, mine, theirs, features, local)

    top, total, target = stats[:, 0], stats[:, 1], stats[:, 2]
    for bit in bits_of(emits):
        other = lax.ppermute(jnp.stack([top, total, target], 1), "emit", xor_pairs(emits, bit))
        new_top = jnp.maximum(top, other[:, 0])
        total = total * jnp.exp(top - new_top) + other[:, 1] * jnp.exp(other[:, 0] - new_top)
        target = target + other[:, 2]
        top = new_top
    loss = (top + jnp.log(total) - target).reshape(slots * samples)
    scale = (jnp.exp(stats[:, 0] - top) / (total * clients))[:, None, :]
    at_label = ((jnp.exp(target - top) / total - 1.0) / clients)[:, None, :]

    block = hidden // (emits * client_size)
    width = min(256, hidden // 2)
    steps = hidden // 2 // width
    halves = [jax.ShapeDtypeStruct((hidden // 4, feat_dim), bf16)] * 2
    at = lambda bit: jnp.stack([bit * steps, where[1]]).astype(jnp.int32)
    slot_of = lambda s: jnp.minimum(s, slots - 1)
    step_of = lambda s: jnp.maximum(s - slots, 0)

    gh, keep_a, send_a = pl.pallas_call(
        functools.partial(head_grad_kernel, block, slots),
        grid_spec=pltpu.PrefetchScalarGridSpec(
            num_scalar_prefetch=1,
            grid=(slots + steps,),
            in_specs=[
                pl.BlockSpec((rows, samples), lambda s, w: (slot_of(s), 0)),
                pl.BlockSpec((1, 1, samples), lambda s, w: (slot_of(s), 0, 0)),
                pl.BlockSpec((1, 1, samples), lambda s, w: (slot_of(s), 0, 0)),
                pl.BlockSpec((1, 1, samples), lambda s, w: (slot_of(s), 0, 0)),
                pl.BlockSpec((samples, feat_dim), lambda s, w: (slot_of(s), 0)),
                pl.BlockSpec((slots * rows, width), lambda s, w: (0, w[0] + step_of(s))),
            ],
            out_specs=[pl.BlockSpec((rows, feat_dim), lambda s, w: (slot_of(s), 0))]
            + [pl.BlockSpec((width // 2, feat_dim), lambda s, w: (step_of(s), 0))] * 2,
            scratch_shapes=[pltpu.VMEM((slots * rows, feat_dim), bf16)],
        ),
        out_shape=[pltpu.HBM((slots * rows, feat_dim), bf16)] + halves,
        compiler_params=params(58),
        cost_estimate=matmul_cost(feat_dim, slots * rows, hidden // 2 + samples, 20 * MIB),
        name="head_grad",
    )(at(1 - where[2]), p, scale, at_label, local, features, code)

    def emit_rest(gh, code):
        return pl.pallas_call(
            functools.partial(emit_grad_kernel, block),
            grid_spec=pltpu.PrefetchScalarGridSpec(
                num_scalar_prefetch=1,
                grid=(steps,),
                in_specs=[
                    whole((slots * rows, feat_dim)),
                    pl.BlockSpec((slots * rows, width), lambda h, w: (0, w[0] + h)),
                ],
                out_specs=[pl.BlockSpec((width // 2, feat_dim), lambda h, w: (h, 0))] * 2,
            ),
            out_shape=halves,
            compiler_params=params(58),
            cost_estimate=matmul_cost(feat_dim, slots * rows, hidden // 2, 12 * MIB),
            name="emit_grad",
        )(at(where[2]), gh, code)

    def code_grad(first, count, gh):
        return pl.pallas_call(
            code_grad_kernel,
            grid=(count,),
            in_specs=[
                pl.BlockSpec((rows, hidden), lambda s: (s + first, 0)),
                whole((hidden, feat_dim)),
                pl.BlockSpec((1, 1, hidden), lambda s: (s + first, 0, 0)),
                pl.BlockSpec((rows, feat_dim), lambda s: (s + first, 0)),
            ],
            out_specs=per_slot((1, hidden)),
            out_shape=jax.ShapeDtypeStruct((count, 1, hidden), bf16),
            compiler_params=params(58),
            cost_estimate=matmul_cost(count * rows, feat_dim, hidden, 3 * count * MIB),
            name="code_grad",
        )(slope, emit_full, pre_slope, gh)

    add = lambda *terms: sum(t.astype(f32) for t in terms).astype(bf16)
    swap_core = lambda v: lax.ppermute(v, "client", xor_pairs(client_size, 1))
    top_bit = emits // 2
    got_a = swap_core(send_a)
    sum_a = add(keep_a, got_a)
    sum_a, code, gh = lax.optimization_barrier((sum_a, code, gh))
    from_pair = lax.ppermute(sum_a, "emit", xor_pairs(emits, top_bit))
    keep_b, send_b = emit_rest(gh, code)
    send_b, gh = lax.optimization_barrier((send_b, gh))
    got_b = swap_core(send_b)
    early = slots // 2
    early_sum = code_grad(0, early, gh)
    value = add(keep_b, got_b, from_pair)
    value, gh = lax.optimization_barrier((value, gh))
    grad_pre = jnp.concatenate([early_sum, code_grad(early, slots - early, gh)])[:, 0]

    emit_bits, client_bits = bits_of(emits)[:-1][::-1], bits_of(client_size)[1:]
    value = value.reshape((2,) * (len(emit_bits) + len(client_bits)) + (block, feat_dim))
    for bit in emit_bits:
        value = halve(value, 0, "emit", emits, bit, emit_index)
    value = halve(value, value.ndim - 3, "client", client_size, client_bits[0], client_index)
    blocks = grad_pre.reshape(slots, emits * client_size, block).transpose(1, 0, 2)
    blocks, value = lax.optimization_barrier((blocks, value))
    value = value.reshape(client_size // 4, block, feat_dim)
    own = client_index // 4
    pieces = [lax.dynamic_index_in_dim(value, own, 0, keepdims=False)]
    for k in range(1, client_size // 4):
        send = lax.dynamic_index_in_dim(value, own ^ k, 0, keepdims=False)
        pieces.append(lax.ppermute(send, "client", xor_pairs(client_size, 4 * k)))
    value = sum(piece.astype(f32) for piece in pieces)
    emit_grad = value

    got = lax.all_to_all(blocks, ("emit", "client"), 0, 0)
    got = got.reshape(emits, clients, block).astype(f32)
    grad_slots = jnp.sum(got, axis=0).astype(bf16)
    grad_client = lax.dot_general(
        picker, grad_slots, (((0,), (0,)), ((), ())), preferred_element_type=f32
    ).astype(bf16)
    trunk_grad = lax.dot_general(
        trunk_in, grad_client, (((0,), (0,)), ((), ())), preferred_element_type=f32
    )
    return (loss, emit_grad, trunk_grad)


def solution(mesh):
    return jax.shard_map(
        per_device,
        mesh=mesh,
        in_specs=(
            P("client", None),
            P("client"),
            P(),
            P(),
            P(None, "client"),
            P("emit", None),
            P("emit", None),
        ),
        out_specs=(P("client"), P(("emit", "client"), None), P(None, ("emit", "client"))),
        check_vma=False,
    )
```

```python
import functools

import jax
import jax.numpy as jnp
from jax import lax
from jax.experimental import pallas as pl
from jax.experimental.pallas import tpu as pltpu
from jax.sharding import PartitionSpec as P

MIB = 1024 * 1024


def params(mib):
    return pltpu.CompilerParams(vmem_limit_bytes=mib * MIB)


def matmul_cost(m, k, n, nbytes):
    return pl.CostEstimate(flops=2 * m * k * n, bytes_accessed=nbytes, transcendentals=0)


def code_kernel(classes, act_ref, table_ref, code_ref, slope_ref, half_ref):
    @pl.when(pl.program_id(0) == 0)
    def _():
        number = lax.broadcasted_iota(jnp.int32, half_ref.shape, 0)
        half = 0.5 * table_ref[...].astype(jnp.float32)
        half_ref[...] = jnp.where(number < classes, half, 0.0)

    y = act_ref[0] + half_ref[...]
    th = jnp.tanh(y)
    up = 1.0 + th
    code_ref[...] = (y * up).astype(jnp.bfloat16)
    slope_ref[...] = (up * (1.0 + y * (1.0 - th))).astype(jnp.bfloat16)


def forward_kernel(classes, where_ref, code_ref, local_ref, mine_ref, theirs_ref, feat_ref, label_ref, p_ref, stat_ref, emit_ref, heads_ref):
    rows, samples = p_ref.shape

    @pl.when(pl.program_id(0) == 0)
    def _():
        size = local_ref.shape[0]
        half = size // 2
        emit_index, core = where_ref[0], where_ref[1]
        emit_ref[pl.ds(pl.multiple_of(emit_index * size, size), size), :] = local_ref[...]
        for j in range(mine_ref.shape[0]):
            base = (emit_index ^ (j + 1)) * size
            first = pl.multiple_of(base + core * half, half)
            second = pl.multiple_of(base + (1 - core) * half, half)
            emit_ref[pl.ds(first, half), :] = mine_ref[j]
            emit_ref[pl.ds(second, half), :] = theirs_ref[j]

    step, last = pl.program_id(0), pl.num_programs(0) - 1

    def make_heads():
        return jnp.dot(
            code_ref[...], emit_ref[...], preferred_element_type=jnp.float32
        ).astype(jnp.bfloat16)

    def make_logits():
        return lax.dot_general(
            heads_ref[...], feat_ref[...], (((1,), (1,)), ((), ())),
            preferred_element_type=jnp.float32,
        )

    def soften(logits):
        number = lax.broadcasted_iota(jnp.int32, (rows, samples), 0)
        target = jnp.sum(jnp.where(number == label_ref[0], logits, 0.0), axis=0, keepdims=True)
        logits = jnp.where(number < classes, logits, -jnp.inf)
        top = jnp.max(logits, axis=0, keepdims=True)
        p = jnp.exp(logits - top)
        p_ref[...] = p.astype(jnp.bfloat16)
        stat_ref[0, 0:1, :] = top
        stat_ref[0, 1:2, :] = jnp.sum(p, axis=0, keepdims=True)
        stat_ref[0, 2:3, :] = target

    @pl.when(step == 0)
    def _():
        heads_ref[...] = make_heads()

    @pl.when((step > 0) & (step < last))
    def _():
        logits = make_logits()
        heads = make_heads()
        soften(logits)
        heads_ref[...] = heads

    @pl.when(step == last)
    def _():
        soften(make_logits())


def store_emit_grad(block, is_first, code, gh, keep_ref, send_ref):
    acc = lax.dot_general(code, gh, (((0,), (0,)), ((), ())), preferred_element_type=jnp.float32)
    width, feat_dim = acc.shape
    acc = acc.reshape(width // (2 * block), 2, block, feat_dim)
    first, second = acc[:, 0].reshape(width // 2, feat_dim), acc[:, 1].reshape(width // 2, feat_dim)
    keep_ref[...] = jnp.where(is_first, first, second).astype(jnp.bfloat16)
    send_ref[...] = jnp.where(is_first, second, first).astype(jnp.bfloat16)


def head_grad_kernel(clients, block, slots, others, where_ref, p_ref, label_ref, stat_ref, *refs):
    feat_ref, code_ref, gh_ref, keep_ref, send_ref, loss_ref, all_ref = refs[others:]
    step = pl.program_id(0)
    rows = p_ref.shape[0]

    @pl.when(step < slots)
    def _():
        parts = [stat_ref, *refs[:others]]
        top = functools.reduce(jnp.maximum, [part[0, 0:1, :] for part in parts])
        total = sum(part[0, 1:2, :] * jnp.exp(part[0, 0:1, :] - top) for part in parts)
        target = sum(part[0, 2:3, :] for part in parts)
        loss_ref[0] = top + jnp.log(total) - target
        scale = jnp.exp(stat_ref[0, 0:1, :] - top) / (total * clients)
        at_label = (jnp.exp(target - top) / total - 1.0) / clients
        number = lax.broadcasted_iota(jnp.int32, p_ref.shape, 0)
        grad = p_ref[...].astype(jnp.float32) * scale
        grad = jnp.where(number == label_ref[0], at_label, grad)
        gh = jnp.dot(
            grad.astype(jnp.bfloat16), feat_ref[...], preferred_element_type=jnp.float32
        ).astype(jnp.bfloat16)
        gh_ref[...] = gh
        all_ref[pl.ds(pl.multiple_of(step * rows, rows), rows), :] = gh

    @pl.when(step >= slots)
    def _():
        store_emit_grad(block, where_ref[1] == 0, code_ref[...], all_ref[...], keep_ref, send_ref)


def store_code_grad(gh, slope_ref, emit_ref, pre_ref, out_ref):
    hidden = emit_ref.shape[0]
    width = min(512, hidden)
    for c in range(hidden // width):
        cols = slice(c * width, (c + 1) * width)
        grad_code = lax.dot_general(
            gh, emit_ref[cols, :], (((1,), (1,)), ((), ())), preferred_element_type=jnp.float32
        )
        slope = slope_ref[:, cols].astype(jnp.float32)
        grad_sum = 0.5 * jnp.sum(grad_code * slope, axis=0, keepdims=True)
        v = 0.5 * pre_ref[0, :, cols]
        th = jnp.tanh(v)
        pre_slope = 0.5 * (1.0 + th) * (1.0 + v * (1.0 - th))
        out_ref[0, :, cols] = (grad_sum * pre_slope).astype(out_ref.dtype)


def code_grad_kernel(slope_ref, emit_ref, pre_ref, gh_ref, out_ref):
    store_code_grad(gh_ref[...], slope_ref, emit_ref, pre_ref, out_ref)


def emit_grad_kernel(block, where_ref, gh_ref, code_ref, keep_ref, send_ref):
    store_emit_grad(block, where_ref[1] == 0, code_ref[...], gh_ref[...], keep_ref, send_ref)


def xor_pairs(size, bit):
    return [(i, i ^ bit) for i in range(size)]


def bits_of(size):
    return [1 << b for b in range(size.bit_length() - 1)]


def gather_emit(local, client_index):
    emits, clients = lax.axis_size("emit"), lax.axis_size("client")
    core = client_index & 1
    half = local.shape[0] // 2
    mine = lax.dynamic_slice_in_dim(local, core * half, half)[None]
    for bit in bits_of(emits):
        mine = jnp.concatenate([mine, lax.ppermute(mine, "emit", xor_pairs(emits, bit))])
    theirs = lax.ppermute(mine[1:], "client", xor_pairs(clients, 1))
    return mine[1:], theirs


def halve(value, dim, axis, size, bit, index):
    own = jnp.where((index & bit) != 0, 1, 0)
    send = lax.dynamic_index_in_dim(value, 1 - own, dim, keepdims=False)
    keep = lax.dynamic_index_in_dim(value, own, dim, keepdims=False)
    got = lax.ppermute(send, axis, xor_pairs(size, bit))
    return (keep.astype(jnp.float32) + got.astype(jnp.float32)).astype(jnp.bfloat16)


def per_device(features, labels, client_ids, trunk_in, trunk_weight, class_table, emit_weight):
    emits, client_size = lax.axis_size("emit"), lax.axis_size("client")
    clients, hidden = trunk_in.shape
    slots = clients // client_size
    classes = class_table.shape[0]
    feat_dim = features.shape[1]
    samples = features.shape[0] // slots
    rows = -(-classes // 128) * 128
    client_index = lax.axis_index("client")
    emit_index = lax.axis_index("emit")
    f32, bf16 = jnp.float32, jnp.bfloat16

    where = jnp.stack([emit_index, client_index & 1, emit_index // (emits // 2)]).astype(jnp.int32)
    pre_cols = jnp.dot(trunk_in, trunk_weight, preferred_element_type=f32).astype(bf16)
    numbers = lax.iota(jnp.int32, clients)
    picker = (client_ids[:, None] == numbers[None, :]).astype(bf16)
    pre_slots = jnp.dot(picker, pre_cols, preferred_element_type=f32).astype(bf16)
    pre_slots, emit_source = lax.optimization_barrier((pre_slots, emit_weight))
    pre_own = lax.all_to_all(
        pre_slots.reshape(client_size, slots, hidden // client_size), "client", 0, 0
    )
    pre_own = pre_own.transpose(1, 0, 2).reshape(slots, hidden).astype(f32)
    mine, theirs = gather_emit(emit_source, client_index)
    act = (0.5 * jax.nn.silu(pre_own))[:, None, :]
    local = labels - emit_index * classes
    local = jnp.where((local >= 0) & (local < classes), local, -1).reshape(slots, 1, samples)

    half = emit_weight.shape[0] // 2
    before = lambda s: jnp.maximum(s - 1, 0)
    once = dict(pipeline_mode=pl.Buffered(1))
    whole = lambda shape: pl.BlockSpec(shape, lambda s, *_: (0,) * len(shape), **once)
    per_slot = lambda shape: pl.BlockSpec((1,) + shape, lambda s, *_: (s, 0, 0))
    row_block = lambda shape: pl.BlockSpec(shape, lambda s, *_: (s, 0))
    make_code = pl.pallas_call(
        functools.partial(code_kernel, classes),
        grid=(slots,),
        in_specs=[per_slot((1, hidden)), whole((rows, hidden))],
        out_specs=[row_block((rows, hidden)), row_block((rows, hidden))],
        out_shape=[pltpu.HBM((slots * rows, hidden), bf16)] * 2,
        scratch_shapes=[pltpu.VMEM((rows, hidden), f32)],
        compiler_params=params(58),
        cost_estimate=pl.CostEstimate(
            flops=int(4e9), bytes_accessed=4 * slots * rows * hidden, transcendentals=0
        ),
        name="code",
    )
    code, slope = make_code(act, class_table)

    p, stats, emit_full = pl.pallas_call(
        functools.partial(forward_kernel, classes),
        grid_spec=pltpu.PrefetchScalarGridSpec(
            num_scalar_prefetch=1,
            grid=(slots + 1,),
            in_specs=[
                pl.BlockSpec((rows, hidden), lambda s, *_: (jnp.minimum(s, slots - 1), 0)),
                whole(emit_weight.shape),
                whole((emits - 1, half, feat_dim)),
                whole((emits - 1, half, feat_dim)),
                pl.BlockSpec((samples, feat_dim), lambda s, *_: (before(s), 0)),
                pl.BlockSpec((1, 1, samples), lambda s, *_: (before(s), 0, 0)),
            ],
            out_specs=[
                pl.BlockSpec((rows, samples), lambda s, *_: (before(s), 0)),
                pl.BlockSpec((1, 3, samples), lambda s, *_: (before(s), 0, 0)),
                pl.BlockSpec((hidden, feat_dim), lambda s, *_: (0, 0)),
            ],
            scratch_shapes=[pltpu.VMEM((rows, feat_dim), bf16)],
        ),
        out_shape=[
            jax.ShapeDtypeStruct((slots * rows, samples), bf16),
            pltpu.HBM((slots, 3, samples), f32),
            pltpu.HBM((hidden, feat_dim), bf16),
        ],
        compiler_params=params(58),
        cost_estimate=matmul_cost(slots * rows, hidden + samples, feat_dim, 30 * MIB),
        name="forward",
    )(where, code, emit_weight, mine, theirs, features, local)

    others = [lax.ppermute(stats, "emit", xor_pairs(emits, j)) for j in range(1, emits)]

    block = hidden // (emits * client_size)
    width = min(256, hidden // 2)
    steps = hidden // 2 // width
    halves = [jax.ShapeDtypeStruct((hidden // 4, feat_dim), bf16)] * 2
    at = lambda bit: jnp.stack([bit * steps, where[1]]).astype(jnp.int32)
    slot_of = lambda s: jnp.minimum(s, slots - 1)
    step_of = lambda s: jnp.maximum(s - slots, 0)

    gh, keep_a, send_a, loss = pl.pallas_call(
        functools.partial(head_grad_kernel, clients, block, slots, emits - 1),
        grid_spec=pltpu.PrefetchScalarGridSpec(
            num_scalar_prefetch=1,
            grid=(slots + steps,),
            in_specs=[
                pl.BlockSpec((rows, samples), lambda s, w: (slot_of(s), 0)),
                pl.BlockSpec((1, 1, samples), lambda s, w: (slot_of(s), 0, 0)),
                *[pl.BlockSpec((1, 3, samples), lambda s, w: (slot_of(s), 0, 0))] * emits,
                pl.BlockSpec((samples, feat_dim), lambda s, w: (slot_of(s), 0)),
                pl.BlockSpec((slots * rows, width), lambda s, w: (0, w[0] + step_of(s))),
            ],
            out_specs=[pl.BlockSpec((rows, feat_dim), lambda s, w: (slot_of(s), 0))]
            + [pl.BlockSpec((width // 2, feat_dim), lambda s, w: (step_of(s), 0))] * 2
            + [pl.BlockSpec((1, 1, samples), lambda s, w: (slot_of(s), 0, 0))],
            scratch_shapes=[pltpu.VMEM((slots * rows, feat_dim), bf16)],
        ),
        out_shape=[pltpu.HBM((slots * rows, feat_dim), bf16)]
        + halves
        + [jax.ShapeDtypeStruct((slots, 1, samples), f32)],
        compiler_params=params(58),
        cost_estimate=matmul_cost(feat_dim, slots * rows, hidden // 2 + samples, 20 * MIB),
        name="head_grad",
    )(at(1 - where[2]), p, local, stats, *others, features, code)
    loss = loss.reshape(slots * samples)

    def emit_rest(gh, code):
        return pl.pallas_call(
            functools.partial(emit_grad_kernel, block),
            grid_spec=pltpu.PrefetchScalarGridSpec(
                num_scalar_prefetch=1,
                grid=(steps,),
                in_specs=[
                    whole((slots * rows, feat_dim)),
                    pl.BlockSpec((slots * rows, width), lambda h, w: (0, w[0] + h)),
                ],
                out_specs=[pl.BlockSpec((width // 2, feat_dim), lambda h, w: (h, 0))] * 2,
            ),
            out_shape=halves,
            compiler_params=params(58),
            cost_estimate=matmul_cost(feat_dim, slots * rows, hidden // 2, 12 * MIB),
            name="emit_grad",
        )(at(where[2]), gh, code)

    def code_grad(first, count, gh):
        return pl.pallas_call(
            code_grad_kernel,
            grid=(count,),
            in_specs=[
                pl.BlockSpec((rows, hidden), lambda s: (s + first, 0)),
                whole((hidden, feat_dim)),
                pl.BlockSpec((1, 1, hidden), lambda s: (s + first, 0, 0)),
                pl.BlockSpec((rows, feat_dim), lambda s: (s + first, 0)),
            ],
            out_specs=per_slot((1, hidden)),
            out_shape=jax.ShapeDtypeStruct((count, 1, hidden), bf16),
            compiler_params=params(58),
            cost_estimate=matmul_cost(count * rows, feat_dim, hidden, 3 * count * MIB),
            name="code_grad",
        )(slope, emit_full, pre_own[:, None, :], gh)

    add = lambda *terms: sum(t.astype(f32) for t in terms).astype(bf16)
    swap_core = lambda v: lax.ppermute(v, "client", xor_pairs(client_size, 1))
    top_bit = emits // 2
    got_a = swap_core(send_a)
    sum_a = add(keep_a, got_a)
    sum_a, code, gh = lax.optimization_barrier((sum_a, code, gh))
    from_pair = lax.ppermute(sum_a, "emit", xor_pairs(emits, top_bit))
    keep_b, send_b = emit_rest(gh, code)
    send_b, gh = lax.optimization_barrier((send_b, gh))
    got_b = swap_core(send_b)
    early = slots // 2
    early_sum = code_grad(0, early, gh)
    value = add(keep_b, got_b, from_pair)
    value, gh = lax.optimization_barrier((value, gh))
    grad_pre = jnp.concatenate([early_sum, code_grad(early, slots - early, gh)])[:, 0]

    emit_bits, client_bits = bits_of(emits)[:-1][::-1], bits_of(client_size)[1:]
    value = value.reshape((2,) * (len(emit_bits) + len(client_bits)) + (block, feat_dim))
    for bit in emit_bits:
        value = halve(value, 0, "emit", emits, bit, emit_index)
    value = halve(value, value.ndim - 3, "client", client_size, client_bits[0], client_index)
    blocks = grad_pre.reshape(slots, emits * client_size, block).transpose(1, 0, 2)
    blocks, value = lax.optimization_barrier((blocks, value))
    value = value.reshape(client_size // 4, block, feat_dim)
    own = client_index // 4
    pieces = [lax.dynamic_index_in_dim(value, own, 0, keepdims=False)]
    for k in range(1, client_size // 4):
        send = lax.dynamic_index_in_dim(value, own ^ k, 0, keepdims=False)
        pieces.append(lax.ppermute(send, "client", xor_pairs(client_size, 4 * k)))
    value = sum(piece.astype(f32) for piece in pieces)
    emit_grad = value

    got = lax.all_to_all(blocks, ("emit", "client"), 0, 0)
    got = got.reshape(emits, clients, block).astype(f32)
    grad_slots = jnp.sum(got, axis=0).astype(bf16)
    grad_client = lax.dot_general(
        picker, grad_slots, (((0,), (0,)), ((), ())), preferred_element_type=f32
    ).astype(bf16)
    trunk_grad = lax.dot_general(
        trunk_in, grad_client, (((0,), (0,)), ((), ())), preferred_element_type=f32
    )
    return (loss, emit_grad, trunk_grad)


def solution(mesh):
    return jax.shard_map(
        per_device,
        mesh=mesh,
        in_specs=(
            P("client", None),
            P("client"),
            P(),
            P(),
            P(None, "client"),
            P("emit", None),
            P("emit", None),
        ),
        out_specs=(P("client"), P(("emit", "client"), None), P(None, ("emit", "client"))),
        check_vma=False,
    )
```
